32 devices in a mesh: blk: 16 (over z, y, core), rhs: 2 (over x).
Axes of the slice: x: 2, y: 2, z: 4, core: 2. Of those that a mesh axis runs over, the one named last changes fastest.
Arguments:
- signal: bfloat16 [131072, 256], P('blk', 'rhs'), may hold values from -6 to 6
- col_factor: bfloat16 [96, 131072], P(None, 'blk'), may hold values from -0.5 to 0.5
- row_factor: bfloat16 [96, 131072], P(None, 'blk'), may hold values from -0.625 to 0.625
- level_factor: bfloat16 [4, 16, 2, 64, 48, 192], P(None, 'blk', None, 'rhs'), may hold values from -0.4375 to 0.4375
- col_leaf_sizes: int32 [16, 128], P('blk'), may hold values from 1 to 128, 8192 in all within a row
- row_leaf_sizes: int32 [16, 128], P('blk'), may hold values from 1 to 128, 8192 in all within a row
- level_order: int32 [4, 16, 128], P(None, 'blk'), may hold values from 0 to 127, each once within a row
Outputs:
- result: bfloat16 [131072, 256], P('blk', 'rhs')
The draws below stay inside these ranges and needn't reach their ends.
Inputs may be any that keep to these rules, and one draw needn't show every extreme that they name: `col_leaf_sizes`: row d lists in order the sizes of the 128 column leaves that cover unknowns d * 8192 to (d + 1) * 8192 - 1; each row sums to 8192 and its largest entry is 128. `row_leaf_sizes`: row d lists in order the sizes of the 128 row leaves that cover unknowns d * 8192 to (d + 1) * 8192 - 1; each row sums to 8192 and its largest entry is 128. Every level_order[l, d, :] is a permutation of 0 to 127.
All inputs are finite; a program needn't handle non-finite values.
Results may differ from the reference program's by a relative error of at most 0.0076.
Values may be sent and summed in bfloat16 or wider, within the bound.
A program may use at most 128 MiB of HBM per device.

```python
import math
import jax
import jax.numpy as jnp
import numpy as np
from jax import lax

K = 48
P_DEV = 8192
LEAVES_DEV = 128
LEAFMAX = 128
LEVELS = 4
COLS_DEV = 64
GROUPS = 16
R = 128
N = 131072
PEER_BLOCKS = 8


def block_levels(own_key, shape, split, least, high):
    def one(axis_at, parts):
        steps = jax.random.uniform(jax.random.fold_in(jax.random.fold_in(own_key, 6), axis_at), (parts,), jnp.float32, least / len(split), high / len(split))
        return jnp.repeat(jnp.exp(steps), shape[axis_at] // parts).reshape((-1,) + (1,) * (len(shape) - axis_at - 1))

    level = one(*split[0])
    for cut in split[1:]:
        level = level * one(*cut)
    return level


def length_profile(count, total, bound, slope):
    loads = [(1 << 20) // math.isqrt(standing ** slope) + 1 for standing in range(2, count + 1)]
    rest, holding = total - bound - (count - 1), [1] * (count - 1)
    while rest > 0:
        movable = [i for i in range(count - 1) if holding[i] < bound]
        whole, budget = sum([loads[i] for i in movable]), rest
        for i in movable:
            more = min(bound - holding[i], max(1, budget * loads[i] // whole), rest)
            holding[i] = holding[i] + more
            rest = rest - more
    return np.array([bound] + holding)


def uneven_parts(stream_key, number_of, total, bound, slope):
    if number_of == 2:
        one = jax.random.randint(stream_key, (), max(1, total - bound), min(bound, total - 1) + 1)
        return jnp.stack([one, total - one])
    tallies = jnp.asarray(length_profile(number_of, total, bound, slope), jnp.int32)
    twos = (number_of - 1) // 2
    giver, receiver = tallies[1:1 + 2 * twos:2], tallies[2:2 + 2 * twos:2]
    margin = jnp.minimum(giver - 1, bound - receiver)
    passed = jax.random.randint(jax.random.fold_in(stream_key, 1), (twos,), 0, 1 << 20) % (margin + 1)
    tallies = tallies.at[1:1 + 2 * twos:2].set(giver - passed).at[2:2 + 2 * twos:2].set(receiver + passed)
    return tallies[jax.random.permutation(jax.random.fold_in(stream_key, 2), number_of)]


def gaussian(key, extent, spread, limit, cuts=(), kind=jnp.bfloat16):
    loudness = block_levels(key, extent, cuts, -0.22, 0.18) if cuts else 1.0
    values = jax.random.normal(key, extent, jnp.float32) * spread * loudness
    return jnp.minimum(jnp.maximum(values, -limit), limit).astype(kind)


def setup_inputs(seed: int = 0) -> dict:
    seeds = jax.random.split(jax.random.key(seed), 8)
    return {
        "signal": gaussian(seeds[0], (N, 2 * R), 1.0, 6.0, ((0, 16), (1, 2))),
        "col_factor": gaussian(seeds[1], (2 * K, N), (2 * P_DEV // LEAVES_DEV) ** -0.5, 0.5, ((1, 16),)),
        "row_factor": gaussian(seeds[2], (2 * K, N), (2 * K) ** -0.5, 0.625, ((1, 16),)),
        "level_factor": gaussian(seeds[3], (LEVELS, GROUPS, 2, LEAVES_DEV // 2, K, 4 * K), (4 * K) ** -0.5, 0.4375, ((1, 16), (3, 2))),
        "col_leaf_sizes": jax.vmap(lambda own: uneven_parts(own, LEAVES_DEV, P_DEV, LEAFMAX, 1))(jax.random.split(seeds[4], GROUPS)).reshape((GROUPS, LEAVES_DEV)).astype(jnp.int32),
        "row_leaf_sizes": jax.vmap(lambda own: uneven_parts(own, LEAVES_DEV, P_DEV, LEAFMAX, 1))(jax.random.split(seeds[5], GROUPS)).reshape((GROUPS, LEAVES_DEV)).astype(jnp.int32),
        "level_order": jax.vmap(lambda own: jax.random.permutation(own, LEAVES_DEV))(jax.random.split(seeds[6], LEVELS * GROUPS)).reshape((LEVELS, GROUPS, LEAVES_DEV)).astype(jnp.int32),
    }


def turn_parts(values, groups):
    pieces = values.reshape(values.shape[:-1] + (groups, 2, values.shape[-1] // (2 * groups)))
    turned = jnp.stack([-pieces[..., 1, :], pieces[..., 0, :]], axis=-2)
    return turned.reshape(values.shape)


def leaf_windows(leaf_sizes):
    leaf_sizes = leaf_sizes.astype(jnp.int32)
    starts = (jnp.cumsum(leaf_sizes) - leaf_sizes).astype(jnp.int32)
    offsets = jnp.arange(LEAFMAX, dtype=jnp.int32)
    window_index = jnp.minimum(starts[:, None] + offsets[None, :], P_DEV - 1).astype(jnp.int32)
    inside = offsets[None, :] < leaf_sizes[:, None]
    return starts, window_index, inside


def leaf_coefficients(operands):
    points, factor, leaf_sizes = operands
    starts, window_index, inside = leaf_windows(leaf_sizes)
    flat_index = window_index.reshape(-1)
    gathered = jnp.take(points, flat_index, axis=0).reshape(LEAVES_DEV, LEAFMAX, points.shape[-1])
    weights = jnp.take(factor, flat_index, axis=1).reshape(2, K, LEAVES_DEV, LEAFMAX)
    weights = jnp.where(inside[None, None], weights, jnp.zeros_like(weights))
    paired = jnp.stack([gathered, turn_parts(gathered, R // COLS_DEV)])
    products = jnp.einsum("tkbi,tbic->bkc", weights.astype(jnp.float32), paired.astype(jnp.float32))
    return products.astype(jnp.bfloat16)


def mix_level(operands):
    arrived, weights = operands
    groups = R // COLS_DEV
    partner = jnp.roll(arrived, LEAVES_DEV // 2, axis=0)
    stacked = jnp.concatenate([arrived, turn_parts(arrived, groups), partner, turn_parts(partner, groups)], axis=1)
    products = jnp.einsum("bkm,bmc->bkc", weights.astype(jnp.float32), stacked.astype(jnp.float32))
    return products.astype(jnp.bfloat16)


def leaf_outputs(operands):
    coefficients, factor, leaf_sizes = operands
    starts, window_index, inside = leaf_windows(leaf_sizes)
    weights = jnp.take(factor, window_index.reshape(-1), axis=1).reshape(2, K, LEAVES_DEV, LEAFMAX)
    paired = jnp.stack([coefficients, turn_parts(coefficients, R // COLS_DEV)])
    leafwise = jnp.einsum("tkbi,tbkc->bic", weights.astype(jnp.float32), paired.astype(jnp.float32))
    points = jnp.arange(P_DEV, dtype=jnp.int32)
    covered = starts[None, :] <= points[:, None]
    leaf_index = (jnp.sum(covered.astype(jnp.int32), axis=1) - 1).astype(jnp.int32)
    leaf_start = jnp.max(jnp.where(covered, starts[None, :], jnp.zeros_like(starts)[None, :]), axis=1).astype(jnp.int32)
    flat_index = (leaf_index * LEAFMAX + points - leaf_start).astype(jnp.int32)
    return jnp.take(leafwise.reshape(-1, leafwise.shape[-1]), flat_index, axis=0).astype(jnp.bfloat16)


def reference(signal, col_factor, row_factor, level_factor, col_leaf_sizes, row_leaf_sizes, level_order):
    columns = signal.shape[-1]
    grouped = signal.reshape(GROUPS, P_DEV, columns)
    col_parts = col_factor.reshape(2 * K, GROUPS, P_DEV).transpose(1, 0, 2)
    coefficients = lax.map(leaf_coefficients, (grouped, col_parts, col_leaf_sizes))
    for layer_index in range(LEVELS):
        chosen = level_order[layer_index].astype(jnp.int32)[:, :, None, None]
        outgoing = jnp.take_along_axis(coefficients, chosen, axis=1)
        arrived = outgoing.reshape(GROUPS, GROUPS, PEER_BLOCKS, K, columns)
        arrived = arrived.transpose(1, 0, 2, 3, 4).reshape(GROUPS, LEAVES_DEV, K, columns)
        weights = level_factor[layer_index].reshape(GROUPS, LEAVES_DEV, K, 4 * K)
        coefficients = lax.map(mix_level, (arrived, weights))
    row_parts = row_factor.reshape(2 * K, GROUPS, P_DEV).transpose(1, 0, 2)
    outputs = lax.map(leaf_outputs, (coefficients, row_parts, row_leaf_sizes))
    return outputs.reshape(N, columns)
```

```python
import functools

import jax
import jax.numpy as jnp
from jax import lax
from jax.experimental import pallas as pl
from jax.experimental.pallas import tpu as pltpu
from jax.sharding import PartitionSpec as P

LANES = 128
ROWS = 16
MESH = pl.DeviceIdType.MESH


def turn(values):
    half = values.shape[-1] // 2
    return jnp.concatenate([-values[:, half:], values[:, :half]], axis=1)


def main_kernel(
    n, sig_hbm, cf_hbm, rf_hbm, lf_hbm, col_sizes_hbm, row_sizes_hbm, order_hbm, leafwise,
    sig, cf, rf, flipped, head, tail, head_in, tail_in, loose, coef, send, arr,
    col_sizes, row_sizes, order, col_start, row_start,
    load_sem, cf_sem, small_sem, w_send, w_recv, a_send, a_recv,
):
    levels, _, depth, rank, _ = head.shape
    width = LANES + loose.shape[-1]
    blocks = coef.shape[0]
    chunks = sig.shape[0]
    per = blocks // n
    half = n // 2
    sources = n // 4
    me = lax.axis_index("blk")
    col = lax.axis_index("rhs")
    side = me // half
    place = lax.rem(me, half)
    bf16 = jnp.bfloat16

    smalls = [
        pltpu.make_async_copy(col_sizes_hbm, col_sizes, small_sem.at[0]),
        pltpu.make_async_copy(order_hbm, order, small_sem.at[1]),
        pltpu.make_async_copy(row_sizes_hbm, row_sizes, small_sem.at[2]),
    ]
    load_sig = pltpu.make_async_copy(sig_hbm, sig, load_sem.at[levels, 0])

    def load_cf(c):
        at = pl.ds(pl.multiple_of(c * LANES, LANES), LANES)
        return pltpu.make_async_copy(cf_hbm.at[:, at], cf.at[c], cf_sem.at[c])

    load_rf = pltpu.make_async_copy(rf_hbm, rf, load_sem.at[levels, 2])

    def loads(l):
        return (
            pltpu.make_async_copy(
                lf_hbm.at[l, :, :, :, pl.ds(0, LANES)], head.at[l], load_sem.at[l, 0]
            ),
            pltpu.make_async_copy(
                lf_hbm.at[l, :, :, :, pl.ds(LANES, width - LANES)], loose.at[l], load_sem.at[l, 1]
            ),
        )

    for copy in smalls:
        copy.start()
    load_sig.start()

    def start_cf(c, carry):
        load_cf(c).start()
        return carry

    lax.fori_loop(0, chunks, start_cf, 0)

    barrier = pltpu.get_barrier_semaphore()

    def greet(k, carry):
        peer = lax.rem(me + k, n)
        pl.semaphore_signal(barrier, inc=1, device_id=(peer, col), device_id_type=MESH)
        return carry

    lax.fori_loop(1, n, greet, 0)
    pl.semaphore_signal(barrier, inc=1, device_id=(me, 1 - col), device_id_type=MESH)

    for copy in smalls:
        copy.wait()

    def add_up(b, carry):
        first, last = carry
        col_start[b] = first
        row_start[b] = last
        return first + col_sizes[0, b], last + row_sizes[0, b]

    lax.fori_loop(0, blocks, add_up, (jnp.int32(0), jnp.int32(0)), unroll=8)

    def weight_copies(l):
        return [
            pltpu.make_async_remote_copy(
                src_ref=ref.at[l],
                dst_ref=into.at[l],
                send_sem=w_send.at[l, at],
                recv_sem=w_recv.at[l, at],
                device_id=(me, 1 - col),
                device_id_type=MESH,
            )
            for at, (ref, into) in enumerate(((head, head_in), (tail, tail_in)))
        ]

    def pack(l):
        def one(i, carry):
            tail[l, i] = jnp.concatenate([loose[l, 0, i], loose[l, 1, i]], axis=1)
            return carry

        lax.fori_loop(0, depth, one, 0, unroll=4)

    def block_copy(par, peer):
        return pltpu.make_async_remote_copy(
            src_ref=send.at[par, peer],
            dst_ref=arr.at[par, me],
            send_sem=a_send.at[par, peer],
            recv_sem=a_recv.at[par, me],
            device_id=(peer, col),
            device_id_type=MESH,
        )

    def arrival(par, source):
        return pltpu.make_async_remote_copy(
            src_ref=send.at[par, source],
            dst_ref=arr.at[par, source],
            send_sem=a_send.at[par, source],
            recv_sem=a_recv.at[par, source],
            device_id=(source, col),
            device_id_type=MESH,
        )

    def across(k):
        return (1 - side) * half + lax.rem(place + k, half)

    def beside(k):
        return side * half + lax.rem(place + k, half)

    def hand_out(par, choose):
        def one(k, inner):
            choose(across(k))
            block_copy(par, across(k)).start()

            @pl.when(k > 0)
            def _():
                choose(beside(k))
                block_copy(par, beside(k)).start()

            return inner

        lax.fori_loop(0, half, one, 0)
        choose(me)
        pltpu.make_async_copy(send.at[par, me], arr.at[par, me], a_recv.at[par, me]).start()

    def sent(par):
        def one(k, inner):
            block_copy(par, lax.rem(me + k, n)).wait_send()
            return inner

        lax.fori_loop(1, n, one, 0)

    window = 2 * LANES
    lane = lax.broadcasted_iota(jnp.int32, (1, window), 1)

    def leaves(peer):
        for q in range(per):
            b = order[0, peer * per + q]
            start = col_start[b]
            end = start + col_sizes[0, b]
            c = jnp.minimum(lax.div(start, LANES), chunks - 2)
            base = c * LANES
            inside = jnp.logical_and(lane >= start - base, lane < end - base)
            keep = jnp.where(inside, 1.0, 0.0).astype(bf16)
            weights = jnp.concatenate([cf[c], cf[c + 1]], axis=1) * keep
            values = jnp.concatenate([sig[c], sig[c + 1]], axis=0)
            sums = jnp.dot(weights, values, preferred_element_type=jnp.float32)
            send[0, peer, q] = (sums[:rank] + turn(sums[rank:])).astype(bf16)

    load_sig.wait()

    def wait_cf(c, carry):
        load_cf(c).wait()
        return carry

    lax.fori_loop(0, chunks, wait_cf, 0)
    for l in range(levels):
        for copy in loads(l):
            copy.start()
    load_rf.start()
    pl.semaphore_wait(barrier, n)
    hand_out(0, leaves)

    for l in range(levels):
        for copy in loads(l):
            copy.wait()
        pack(l)
        for copy in weight_copies(l):
            copy.start()
    load_rf.wait()

    def flip(c, inner):
        at = pl.ds(pl.multiple_of(c * LANES, LANES), LANES)
        rows = LANES // ROWS
        flipped[pl.ds(c * rows, rows)] = rf[:, at].T.reshape(rows, ROWS, 2 * rank)
        return inner

    lax.fori_loop(0, chunks, flip, 0, unroll=4)

    blank = jnp.zeros((2 * LANES - width, LANES), bf16)

    def combine(l, par, put):
        def pairs(owner, first, second):
            def one(k, inner):
                at = lax.rem(place + sources - k, sources)
                s = owner * sources + at
                arrival(par, s).wait_recv()
                arrival(par, s + half).wait_recv()
                for q in range(per):
                    i = at * per + q
                    x = arr[par, s, q]
                    y = arr[par, s + half, q]
                    jx = turn(x)
                    jy = turn(y)
                    rest = second[l, i]
                    upper = jnp.concatenate([first[l, 0, i], rest], axis=1)
                    lower = jnp.concatenate([first[l, 1, i], rest], axis=1)
                    cut = LANES - 2 * rank
                    over = jnp.concatenate([x, jx, y, jy, blank], axis=0)
                    under = jnp.concatenate([y, jy, x[:cut], blank, x[cut:], jx], axis=0)
                    put(s * per + q, jnp.dot(
                        upper, over, preferred_element_type=jnp.float32
                    ).astype(bf16))
                    put((s + half) * per + q, jnp.dot(
                        lower, under, preferred_element_type=jnp.float32
                    ).astype(bf16))
                return inner

            lax.fori_loop(0, sources, one, 0)

        pairs(col, head, tail)
        for copy in weight_copies(l):
            copy.wait_recv()
        pairs(1 - col, head_in, tail_in)

    def keep_block(b, values):
        coef[b] = values

    def level(l, carry):
        par = lax.rem(l, 2)
        combine(l, par, keep_block)

        @pl.when(l > 0)
        def _():
            sent(1 - par)

        def choose(peer):
            for q in range(per):
                send[1 - par, peer, q] = coef[order[l + 1, peer * per + q]]

        hand_out(1 - par, choose)
        return carry

    lax.fori_loop(0, levels - 1, level, 0)

    reach = leafwise.shape[1]

    def put_rows(b, values):
        base = lax.div(row_start[b], ROWS)
        rows = [flipped[base + i] for i in range(reach // ROWS)]
        pair = jnp.concatenate([values, turn(values)], axis=0)
        leafwise[b] = jnp.dot(
            jnp.concatenate(rows, axis=0), pair, preferred_element_type=jnp.float32
        ).astype(bf16)

    last = (levels - 1) % 2
    combine(levels - 1, last, put_rows)
    sent(1 - last)
    sent(last)
    for l in range(levels):
        for copy in weight_copies(l):
            copy.wait_send()


def rows_kernel(sizes, leafwise, out_hbm, out, sem):
    blocks, reach, _ = leafwise.shape
    points = out_hbm.shape[0]
    parts = sem.shape[0]
    chunk = points // parts
    group = 8
    row = lax.broadcasted_iota(jnp.int32, (ROWS, LANES), 0)

    def part(c):
        at = pl.ds(pl.multiple_of(c * chunk, chunk), chunk)
        return pltpu.make_async_copy(out.at[at], out_hbm.at[at], sem.at[c])

    def leaves(g, begin):
        start = begin
        for i in range(group):
            b = g * group + i
            base = pl.multiple_of(start // ROWS * ROWS, ROWS)
            before = out[pl.ds(base, ROWS), :]
            top = jnp.where(row < start - base, before, leafwise[b, pl.ds(0, ROWS), :])
            out[pl.ds(base, ROWS), :] = top
            out[pl.ds(base + ROWS, reach - ROWS), :] = leafwise[b, pl.ds(ROWS, reach - ROWS), :]
            start = start + sizes[0, b]

        return start

    lax.fori_loop(0, blocks // group, leaves, jnp.int32(0))
    for c in range(parts):
        part(c).start()
    for c in range(parts):
        part(c).wait()


def local(
    n, signal, col_factor, row_factor, level_factor, col_leaf_sizes, row_leaf_sizes, level_order
):
    levels, _, halves, depth, rank, width = level_factor.shape
    blocks = col_leaf_sizes.shape[1]
    points, columns = signal.shape
    per = blocks // n
    bf16 = jnp.bfloat16
    smem = pl.BlockSpec(memory_space=pltpu.SMEM)
    vmem = pl.BlockSpec(memory_space=pltpu.VMEM)
    hbm = pl.BlockSpec(memory_space=pltpu.HBM)
    reach = LANES + ROWS
    factors = level_factor.reshape(levels, halves, depth, rank, width)
    leafwise = pl.pallas_call(
        functools.partial(main_kernel, n),
        out_shape=pltpu.VMEM((blocks, reach, columns), bf16),
        in_specs=[hbm] * 7,
        out_specs=vmem,
        scratch_shapes=[
            pltpu.VMEM((points // LANES, LANES, columns), bf16),
            pltpu.VMEM((points // LANES, 2 * rank, LANES), bf16),
            pltpu.VMEM((2 * rank, points), bf16),
            pltpu.VMEM(((points + reach) // ROWS, ROWS, 2 * rank), bf16),
            pltpu.VMEM((levels, halves, depth, rank, LANES), bf16),
            pltpu.VMEM((levels, depth, rank, LANES), bf16),
            pltpu.VMEM((levels, halves, depth, rank, LANES), bf16),
            pltpu.VMEM((levels, depth, rank, LANES), bf16),
            pltpu.VMEM((levels, halves, depth, rank, width - LANES), bf16),
            pltpu.VMEM((blocks, rank, columns), bf16),
            pltpu.VMEM((2, n, per, rank, columns), bf16),
            pltpu.VMEM((2, n, per, rank, columns), bf16),
            pltpu.SMEM((1, blocks), jnp.int32),
            pltpu.SMEM((1, blocks), jnp.int32),
            pltpu.SMEM((levels, blocks), jnp.int32),
            pltpu.SMEM((blocks,), jnp.int32),
            pltpu.SMEM((blocks,), jnp.int32),
            pltpu.SemaphoreType.DMA((levels + 1, 3)),
            pltpu.SemaphoreType.DMA((points // LANES,)),
            pltpu.SemaphoreType.DMA((3,)),
            pltpu.SemaphoreType.DMA((levels, 2)),
            pltpu.SemaphoreType.DMA((levels, 2)),
            pltpu.SemaphoreType.DMA((2, n)),
            pltpu.SemaphoreType.DMA((2, n)),
        ],
        compiler_params=pltpu.CompilerParams(
            collective_id=0, has_side_effects=True, vmem_limit_bytes=58000000
        ),
        name="levels",
    )(
        signal.reshape(points // LANES, LANES, columns), col_factor, row_factor, factors, col_leaf_sizes, row_leaf_sizes,
        level_order.reshape(levels, blocks),
    )
    return pl.pallas_call(
        rows_kernel,
        out_shape=jax.ShapeDtypeStruct((points, columns), bf16),
        in_specs=[smem, vmem],
        out_specs=hbm,
        scratch_shapes=[
            pltpu.VMEM((points + reach, columns), bf16),
            pltpu.SemaphoreType.DMA((8,)),
        ],
        compiler_params=pltpu.CompilerParams(vmem_limit_bytes=16 << 20),
        name="rows",
    )(row_leaf_sizes, leafwise)


def solution(mesh):
    in_specs = (
        P("blk", "rhs"),
        P(None, "blk"),
        P(None, "blk"),
        P(None, "blk", None, "rhs", None, None),
        P("blk", None),
        P("blk", None),
        P(None, "blk", None),
    )
    return jax.shard_map(
        functools.partial(local, mesh.shape["blk"]),
        mesh=mesh, in_specs=in_specs, out_specs=P("blk", "rhs"), check_vma=False,
    )
```

```python
import functools

import jax
import jax.numpy as jnp
from jax import lax
from jax.experimental import pallas as pl
from jax.experimental.pallas import tpu as pltpu
from jax.sharding import PartitionSpec as P

LANES = 128
ROWS = 16
MESH = pl.DeviceIdType.MESH


def turn(values):
    half = values.shape[-1] // 2
    return jnp.concatenate([-values[:, half:], values[:, :half]], axis=1)


def main_kernel(
    n, sig_hbm, cf_hbm, rf_hbm, lf_hbm, col_sizes_hbm, row_sizes_hbm, order_hbm, leafwise,
    sig, cf, rf, flipped, head, tail, head_in, tail_in, loose, coef, send, arr,
    col_sizes, row_sizes, order, col_start, row_start,
    load_sem, cf_sem, small_sem, w_send, w_recv, a_send, a_recv,
):
    levels, _, depth, rank, _ = head.shape
    width = LANES + loose.shape[-1]
    blocks = coef.shape[0]
    chunks = sig.shape[0]
    per = blocks // n
    half = n // 2
    sources = n // 4
    me = lax.axis_index("blk")
    col = lax.axis_index("rhs")
    side = me // half
    place = lax.rem(me, half)
    bf16 = jnp.bfloat16

    smalls = [
        pltpu.make_async_copy(col_sizes_hbm, col_sizes, small_sem.at[0]),
        pltpu.make_async_copy(order_hbm, order, small_sem.at[1]),
        pltpu.make_async_copy(row_sizes_hbm, row_sizes, small_sem.at[2]),
    ]
    load_sig = pltpu.make_async_copy(sig_hbm, sig, load_sem.at[levels, 0])

    def load_cf(c):
        at = pl.ds(pl.multiple_of(c * LANES, LANES), LANES)
        return pltpu.make_async_copy(cf_hbm.at[:, at], cf.at[c], cf_sem.at[c])

    load_rf = pltpu.make_async_copy(rf_hbm, rf, load_sem.at[levels, 2])

    def loads(l):
        return (
            pltpu.make_async_copy(
                lf_hbm.at[l, :, :, :, pl.ds(0, LANES)], head.at[l], load_sem.at[l, 0]
            ),
            pltpu.make_async_copy(
                lf_hbm.at[l, :, :, :, pl.ds(LANES, width - LANES)], loose.at[l], load_sem.at[l, 1]
            ),
        )

    for copy in smalls:
        copy.start()
    load_sig.start()

    def start_cf(c, carry):
        load_cf(c).start()
        return carry

    lax.fori_loop(0, chunks, start_cf, 0)

    barrier = pltpu.get_barrier_semaphore()

    def greet(k, carry):
        peer = lax.rem(me + k, n)
        pl.semaphore_signal(barrier, inc=1, device_id=(peer, col), device_id_type=MESH)
        return carry

    lax.fori_loop(1, n, greet, 0)
    pl.semaphore_signal(barrier, inc=1, device_id=(me, 1 - col), device_id_type=MESH)

    for copy in smalls:
        copy.wait()

    def add_up(b, carry):
        first, last = carry
        col_start[b] = first
        row_start[b] = last
        return first + col_sizes[0, b], last + row_sizes[0, b]

    lax.fori_loop(0, blocks, add_up, (jnp.int32(0), jnp.int32(0)), unroll=8)

    def weight_copies(l):
        return [
            pltpu.make_async_remote_copy(
                src_ref=ref.at[l],
                dst_ref=into.at[l],
                send_sem=w_send.at[l, at],
                recv_sem=w_recv.at[l, at],
                device_id=(me, 1 - col),
                device_id_type=MESH,
            )
            for at, (ref, into) in enumerate(((head, head_in), (tail, tail_in)))
        ]

    def pack(l):
        def one(i, carry):
            tail[l, i] = jnp.concatenate([loose[l, 0, i], loose[l, 1, i]], axis=1)
            return carry

        lax.fori_loop(0, depth, one, 0, unroll=4)

    def block_copy(par, peer):
        return pltpu.make_async_remote_copy(
            src_ref=send.at[par, peer],
            dst_ref=arr.at[par, me],
            send_sem=a_send.at[par, peer],
            recv_sem=a_recv.at[par, me],
            device_id=(peer, col),
            device_id_type=MESH,
        )

    def arrival(par, source):
        return pltpu.make_async_remote_copy(
            src_ref=send.at[par, source],
            dst_ref=arr.at[par, source],
            send_sem=a_send.at[par, source],
            recv_sem=a_recv.at[par, source],
            device_id=(source, col),
            device_id_type=MESH,
        )

    def across(k):
        return (1 - side) * half + lax.rem(place + k, half)

    def beside(k):
        return side * half + lax.rem(place + k, half)

    def hand_out(par, choose):
        def one(k, inner):
            choose(across(k))
            block_copy(par, across(k)).start()

            @pl.when(k > 0)
            def _():
                choose(beside(k))
                block_copy(par, beside(k)).start()

            return inner

        lax.fori_loop(0, half, one, 0)
        choose(me)
        pltpu.make_async_copy(send.at[par, me], arr.at[par, me], a_recv.at[par, me]).start()

    def sent(par):
        def one(k, inner):
            block_copy(par, lax.rem(me + k, n)).wait_send()
            return inner

        lax.fori_loop(1, n, one, 0)

    window = 2 * LANES
    lane = lax.broadcasted_iota(jnp.int32, (1, window), 1)

    def leaves(peer):
        for q in range(per):
            b = order[0, peer * per + q]
            start = col_start[b]
            end = start + col_sizes[0, b]
            c = jnp.minimum(lax.div(start, LANES), chunks - 2)
            base = c * LANES
            inside = jnp.logical_and(lane >= start - base, lane < end - base)
            keep = jnp.where(inside, 1.0, 0.0).astype(bf16)
            weights = jnp.concatenate([cf[c], cf[c + 1]], axis=1) * keep
            values = jnp.concatenate([sig[c], sig[c + 1]], axis=0)
            sums = jnp.dot(weights, values, preferred_element_type=jnp.float32)
            send[0, peer, q] = (sums[:rank] + turn(sums[rank:])).astype(bf16)

    load_sig.wait()

    def wait_cf(c, carry):
        load_cf(c).wait()
        return carry

    lax.fori_loop(0, chunks, wait_cf, 0)
    for l in range(levels):
        for copy in loads(l):
            copy.start()
    load_rf.start()
    pl.semaphore_wait(barrier, n)
    loads(0)[0].wait()
    weight_copies(0)[0].start()
    hand_out(0, leaves)

    for l in range(levels):
        for copy in loads(l)[l == 0:]:
            copy.wait()
        pack(l)
        for copy in weight_copies(l)[l == 0:]:
            copy.start()
    load_rf.wait()

    def flip(c, inner):
        at = pl.ds(pl.multiple_of(c * LANES, LANES), LANES)
        rows = LANES // ROWS
        flipped[pl.ds(c * rows, rows)] = rf[:, at].T.reshape(rows, ROWS, 2 * rank)
        return inner

    lax.fori_loop(0, chunks, flip, 0, unroll=4)

    blank = jnp.zeros((2 * LANES - width, LANES), bf16)

    def blend(l, par, s, at, first, second):
        arrival(par, s).wait_recv()
        arrival(par, s + half).wait_recv()
        for q in range(per):
            i = at * per + q
            x = arr[par, s, q]
            y = arr[par, s + half, q]
            jx = turn(x)
            jy = turn(y)
            rest = second[l, i]
            upper = jnp.concatenate([first[l, 0, i], rest], axis=1)
            lower = jnp.concatenate([first[l, 1, i], rest], axis=1)
            cut = LANES - 2 * rank
            over = jnp.concatenate([x, jx, y, jy, blank], axis=0)
            under = jnp.concatenate([y, jy, x[:cut], blank, x[cut:], jx], axis=0)
            coef[s * per + q] = jnp.dot(
                upper, over, preferred_element_type=jnp.float32
            ).astype(bf16)
            coef[(s + half) * per + q] = jnp.dot(
                lower, under, preferred_element_type=jnp.float32
            ).astype(bf16)

    def weights_here(l):
        for copy in weight_copies(l):
            copy.wait_recv()

    def combine_first(par):
        def pairs(owner, first, second):
            def one(k, inner):
                at = lax.rem(place + sources - k, sources)
                blend(0, par, owner * sources + at, at, first, second)
                return inner

            lax.fori_loop(0, sources, one, 0)

        pairs(col, head, tail)
        weights_here(0)
        pairs(1 - col, head_in, tail_in)

    def combine(l, par, after=None):
        weights_here(l)

        def one(k, inner):
            s = lax.rem(place + half - k, half)
            at = lax.rem(s, sources)
            own = s // sources == col

            @pl.when(own)
            def _():
                blend(l, par, s, at, head, tail)

            @pl.when(jnp.logical_not(own))
            def _():
                blend(l, par, s, at, head_in, tail_in)

            if after is not None:
                after(s)
            return inner

        lax.fori_loop(0, half, one, 0)

    def pass_on(l, par):
        def choose(peer):
            for q in range(per):
                send[1 - par, peer, q] = coef[order[l + 1, peer * per + q]]

        hand_out(1 - par, choose)

    combine_first(0)
    pass_on(0, 0)

    def level(l, carry):
        par = lax.rem(l, 2)
        combine(l, par)
        sent(1 - par)
        pass_on(l, par)
        return carry

    lax.fori_loop(1, levels - 1, level, 0)

    reach = leafwise.shape[1]

    def rows(s):
        for b in [t * per + q for t in (s, s + half) for q in range(per)]:
            base = lax.div(row_start[b], ROWS)
            window = [flipped[base + i] for i in range(reach // ROWS)]
            values = coef[b]
            pair = jnp.concatenate([values, turn(values)], axis=0)
            leafwise[b] = jnp.dot(
                jnp.concatenate(window, axis=0), pair, preferred_element_type=jnp.float32
            ).astype(bf16)

    last = (levels - 1) % 2
    combine(levels - 1, last, rows)
    sent(1 - last)
    sent(last)
    for l in range(levels):
        for copy in weight_copies(l):
            copy.wait_send()


def rows_kernel(sizes, leafwise, out_hbm, out, sem):
    blocks, reach, _ = leafwise.shape
    points = out_hbm.shape[0]
    parts = sem.shape[0]
    chunk = points // parts
    group = 8
    row = lax.broadcasted_iota(jnp.int32, (ROWS, LANES), 0)

    def part(c):
        at = pl.ds(pl.multiple_of(c * chunk, chunk), chunk)
        return pltpu.make_async_copy(out.at[at], out_hbm.at[at], sem.at[c])

    def leaves(g, begin):
        start = begin
        for i in range(group):
            b = g * group + i
            base = pl.multiple_of(start // ROWS * ROWS, ROWS)
            before = out[pl.ds(base, ROWS), :]
            top = jnp.where(row < start - base, before, leafwise[b, pl.ds(0, ROWS), :])
            out[pl.ds(base, ROWS), :] = top
            out[pl.ds(base + ROWS, reach - ROWS), :] = leafwise[b, pl.ds(ROWS, reach - ROWS), :]
            start = start + sizes[0, b]

        @pl.when(start // chunk > begin // chunk)
        def _():
            part(begin // chunk).start()

        return start

    lax.fori_loop(0, blocks // group, leaves, jnp.int32(0))
    for c in range(parts):
        part(c).wait()


def local(
    n, signal, col_factor, row_factor, level_factor, col_leaf_sizes, row_leaf_sizes, level_order
):
    levels, _, halves, depth, rank, width = level_factor.shape
    blocks = col_leaf_sizes.shape[1]
    points, columns = signal.shape
    per = blocks // n
    bf16 = jnp.bfloat16
    smem = pl.BlockSpec(memory_space=pltpu.SMEM)
    vmem = pl.BlockSpec(memory_space=pltpu.VMEM)
    hbm = pl.BlockSpec(memory_space=pltpu.HBM)
    reach = LANES + ROWS
    factors = level_factor.reshape(levels, halves, depth, rank, width)
    leafwise = pl.pallas_call(
        functools.partial(main_kernel, n),
        out_shape=pltpu.VMEM((blocks, reach, columns), bf16),
        in_specs=[hbm] * 7,
        out_specs=vmem,
        scratch_shapes=[
            pltpu.VMEM((points // LANES, LANES, columns), bf16),
            pltpu.VMEM((points // LANES, 2 * rank, LANES), bf16),
            pltpu.VMEM((2 * rank, points), bf16),
            pltpu.VMEM(((points + reach) // ROWS, ROWS, 2 * rank), bf16),
            pltpu.VMEM((levels, halves, depth, rank, LANES), bf16),
            pltpu.VMEM((levels, depth, rank, LANES), bf16),
            pltpu.VMEM((levels, halves, depth, rank, LANES), bf16),
            pltpu.VMEM((levels, depth, rank, LANES), bf16),
            pltpu.VMEM((levels, halves, depth, rank, width - LANES), bf16),
            pltpu.VMEM((blocks, rank, columns), bf16),
            pltpu.VMEM((2, n, per, rank, columns), bf16),
            pltpu.VMEM((2, n, per, rank, columns), bf16),
            pltpu.SMEM((1, blocks), jnp.int32),
            pltpu.SMEM((1, blocks), jnp.int32),
            pltpu.SMEM((levels, blocks), jnp.int32),
            pltpu.SMEM((blocks,), jnp.int32),
            pltpu.SMEM((blocks,), jnp.int32),
            pltpu.SemaphoreType.DMA((levels + 1, 3)),
            pltpu.SemaphoreType.DMA((points // LANES,)),
            pltpu.SemaphoreType.DMA((3,)),
            pltpu.SemaphoreType.DMA((levels, 2)),
            pltpu.SemaphoreType.DMA((levels, 2)),
            pltpu.SemaphoreType.DMA((2, n)),
            pltpu.SemaphoreType.DMA((2, n)),
        ],
        compiler_params=pltpu.CompilerParams(
            collective_id=0, has_side_effects=True, vmem_limit_bytes=58000000
        ),
        name="levels",
    )(
        signal.reshape(points // LANES, LANES, columns), col_factor, row_factor, factors, col_leaf_sizes, row_leaf_sizes,
        level_order.reshape(levels, blocks),
    )
    return pl.pallas_call(
        rows_kernel,
        out_shape=jax.ShapeDtypeStruct((points, columns), bf16),
        in_specs=[smem, vmem],
        out_specs=hbm,
        scratch_shapes=[
            pltpu.VMEM((points + reach, columns), bf16),
            pltpu.SemaphoreType.DMA((8,)),
        ],
        compiler_params=pltpu.CompilerParams(vmem_limit_bytes=16 << 20),
        name="rows",
    )(row_leaf_sizes, leafwise)


def solution(mesh):
    in_specs = (
        P("blk", "rhs"),
        P(None, "blk"),
        P(None, "blk"),
        P(None, "blk", None, "rhs", None, None),
        P("blk", None),
        P("blk", None),
        P(None, "blk", None),
    )
    return jax.shard_map(
        functools.partial(local, mesh.shape["blk"]),
        mesh=mesh, in_specs=in_specs, out_specs=P("blk", "rhs"), check_vma=False,
    )
```

```python
import functools

import jax
import jax.numpy as jnp
from jax import lax
from jax.experimental import pallas as pl
from jax.experimental.pallas import tpu as pltpu
from jax.sharding import PartitionSpec as P

LANES = 128
ROWS = 16
MESH = pl.DeviceIdType.MESH


def turn(values):
    half = values.shape[-1] // 2
    return jnp.concatenate([-values[:, half:], values[:, :half]], axis=1)


def main_kernel(
    n, sig_hbm, cf_hbm, rf_hbm, lf_hbm, col_sizes_hbm, row_sizes_hbm, order_hbm, leafwise,
    sig, cf, rf, flipped, head, tail, head_in, tail_in, loose, mixed, send, arr,
    col_sizes, row_sizes, order, col_start, row_start,
    load_sem, cf_sem, small_sem, w_send, w_recv, a_send, a_recv,
):
    levels, _, depth, rank, _ = head.shape
    width = LANES + loose.shape[-1]
    blocks = mixed.shape[2]
    chunks = sig.shape[0]
    per = blocks // n
    half = n // 2
    sources = n // 4
    me = lax.axis_index("blk")
    col = lax.axis_index("rhs")
    side = me // half
    place = lax.rem(me, half)
    bf16 = jnp.bfloat16

    smalls = [
        pltpu.make_async_copy(col_sizes_hbm, col_sizes, small_sem.at[0]),
        pltpu.make_async_copy(order_hbm, order, small_sem.at[1]),
        pltpu.make_async_copy(row_sizes_hbm, row_sizes, small_sem.at[2]),
    ]
    load_sig = pltpu.make_async_copy(sig_hbm, sig, load_sem.at[levels, 0])

    def load_cf(c):
        at = pl.ds(pl.multiple_of(c * LANES, LANES), LANES)
        return pltpu.make_async_copy(cf_hbm.at[:, at], cf.at[c], cf_sem.at[c])

    load_rf = pltpu.make_async_copy(rf_hbm, rf, load_sem.at[levels, 2])

    def loads(l):
        return (
            pltpu.make_async_copy(
                lf_hbm.at[l, :, :, :, pl.ds(0, LANES)], head.at[l], load_sem.at[l, 0]
            ),
            pltpu.make_async_copy(
                lf_hbm.at[l, :, :, :, pl.ds(LANES, width - LANES)], loose.at[l], load_sem.at[l, 1]
            ),
        )

    for copy in smalls:
        copy.start()
    load_sig.start()

    def start_cf(c, carry):
        load_cf(c).start()
        return carry

    lax.fori_loop(0, chunks, start_cf, 0)

    barrier = pltpu.get_barrier_semaphore()

    def greet(k, carry):
        peer = lax.rem(me + k, n)
        pl.semaphore_signal(barrier, inc=1, device_id=(peer, col), device_id_type=MESH)
        return carry

    lax.fori_loop(1, n, greet, 0)
    pl.semaphore_signal(barrier, inc=1, device_id=(me, 1 - col), device_id_type=MESH)

    for copy in smalls:
        copy.wait()

    def add_up(b, carry):
        first, last = carry
        col_start[b] = first
        row_start[b] = last
        return first + col_sizes[0, b], last + row_sizes[0, b]

    lax.fori_loop(0, blocks, add_up, (jnp.int32(0), jnp.int32(0)), unroll=8)

    def weight_copies(l):
        return [
            pltpu.make_async_remote_copy(
                src_ref=ref.at[l],
                dst_ref=into.at[l],
                send_sem=w_send.at[l, at],
                recv_sem=w_recv.at[l, at],
                device_id=(me, 1 - col),
                device_id_type=MESH,
            )
            for at, (ref, into) in enumerate(((head, head_in), (tail, tail_in)))
        ]

    def pack(l):
        def one(i, carry):
            tail[l, i] = jnp.concatenate([loose[l, 0, i], loose[l, 1, i]], axis=1)
            return carry

        lax.fori_loop(0, depth, one, 0, unroll=4)

    def block_copy(t, par, peer):
        return pltpu.make_async_remote_copy(
            src_ref=send.at[t, par, peer],
            dst_ref=arr.at[t, par, me],
            send_sem=a_send.at[t, par, peer],
            recv_sem=a_recv.at[t, par, me],
            device_id=(peer, col),
            device_id_type=MESH,
        )

    def arrival(t, par, source):
        return pltpu.make_async_remote_copy(
            src_ref=send.at[t, par, source],
            dst_ref=arr.at[t, par, source],
            send_sem=a_send.at[t, par, source],
            recv_sem=a_recv.at[t, par, source],
            device_id=(source, col),
            device_id_type=MESH,
        )

    def across(k):
        return (1 - side) * half + lax.rem(place + k, half)

    def beside(k):
        return side * half + lax.rem(place + k, half)

    def hand_out(t, par, choose):
        def one(k, inner):
            choose(across(k))
            block_copy(t, par, across(k)).start()

            @pl.when(k > 0)
            def _():
                choose(beside(k))
                block_copy(t, par, beside(k)).start()

            return inner

        lax.fori_loop(0, half, one, 0)
        choose(me)
        pltpu.make_async_copy(
            send.at[t, par, me], arr.at[t, par, me], a_recv.at[t, par, me]
        ).start()

    def sent(t, par):
        def one(k, inner):
            block_copy(t, par, lax.rem(me + k, n)).wait_send()
            return inner

        lax.fori_loop(1, n, one, 0)

    quarter = LANES // 4
    first_slot = lax.rem(lax.broadcasted_iota(jnp.int32, (rank, LANES), 1), 2 * quarter) < quarter

    def left(values):
        return pltpu.roll(values, LANES - quarter, 1)

    def right(values):
        return pltpu.roll(values, quarter, 1)

    window = 2 * LANES
    lane = lax.broadcasted_iota(jnp.int32, (1, window), 1)

    def leaves(peer):
        blocks_of = []
        for q in range(per):
            b = order[0, peer * per + q]
            start = col_start[b]
            end = start + col_sizes[0, b]
            c = jnp.minimum(lax.div(start, LANES), chunks - 2)
            base = c * LANES
            inside = jnp.logical_and(lane >= start - base, lane < end - base)
            keep = jnp.where(inside, 1.0, 0.0).astype(bf16)
            weights = jnp.concatenate([cf[c], cf[c + 1]], axis=1) * keep
            values = jnp.concatenate([sig[c], sig[c + 1]], axis=0)
            sums = jnp.dot(weights, values, preferred_element_type=jnp.float32)
            blocks_of.append(sums[:rank] + turn(sums[rank:]))
        for u in range(per // 2):
            one, two = blocks_of[2 * u], blocks_of[2 * u + 1]
            send[0, 0, peer, u] = jnp.where(first_slot, one, right(two)).astype(bf16)
            send[1, 0, peer, u] = jnp.where(first_slot, left(one), two).astype(bf16)

    load_sig.wait()

    def wait_cf(c, carry):
        load_cf(c).wait()
        return carry

    lax.fori_loop(0, chunks, wait_cf, 0)
    for l in range(levels):
        for copy in loads(l):
            copy.start()
    load_rf.start()
    pl.semaphore_wait(barrier, n)
    loads(0)[0].wait()
    weight_copies(0)[0].start()
    hand_out(0, 0, leaves)
    hand_out(1, 0, lambda peer: None)

    for l in range(levels):
        for copy in loads(l)[l == 0:]:
            copy.wait()
        pack(l)
        for copy in weight_copies(l)[l == 0:]:
            copy.start()
    load_rf.wait()

    def flip(c, inner):
        at = pl.ds(pl.multiple_of(c * LANES, LANES), LANES)
        rows = LANES // ROWS
        flipped[pl.ds(c * rows, rows)] = rf[:, at].T.reshape(rows, ROWS, 2 * rank)
        return inner

    lax.fori_loop(0, chunks, flip, 0, unroll=4)

    blank = jnp.zeros((2 * LANES - width, LANES), bf16)

    def keep(t, j, sums):
        pair = jnp.where(first_slot, sums[:rank], sums[rank:])
        both = pair.astype(bf16)
        mixed[t, 0, j] = both
        mixed[t, 1, j + 1] = both
        mixed[t, 0, j + 1] = left(pair).astype(bf16)
        mixed[t, 1, j] = right(pair).astype(bf16)

    def blend(t, l, par, s, at, first, second):
        arrival(t, par, s).wait_recv()
        arrival(t, par, s + half).wait_recv()
        for u in range(per // 2):
            i = at * per + 2 * u
            x = arr[t, par, s, u]
            y = arr[t, par, s + half, u]
            jx = turn(x)
            jy = turn(y)

            def weights(h):
                return jnp.concatenate([
                    jnp.concatenate([first[l, h, i], second[l, i]], axis=1),
                    jnp.concatenate([first[l, h, i + 1], second[l, i + 1]], axis=1),
                ], axis=0)

            cut = LANES - 2 * rank
            over = jnp.concatenate([x, jx, y, jy, blank], axis=0)
            under = jnp.concatenate([y, jy, x[:cut], blank, x[cut:], jx], axis=0)
            keep(t, s * per + 2 * u, jnp.dot(
                weights(0), over, preferred_element_type=jnp.float32
            ))
            keep(t, (s + half) * per + 2 * u, jnp.dot(
                weights(1), under, preferred_element_type=jnp.float32
            ))

    def weights_here(l):
        for copy in weight_copies(l):
            copy.wait_recv()

    def pairs(t, owner, first, second):
        def one(k, inner):
            at = lax.rem(place + sources - k, sources)
            blend(t, 0, 0, owner * sources + at, at, first, second)
            return inner

        lax.fori_loop(0, sources, one, 0)

    def combine(t, l, par, after=None):
        def one(k, inner):
            s = lax.rem(place + half - k, half)
            at = lax.rem(s, sources)
            own = s // sources == col

            @pl.when(own)
            def _():
                blend(t, l, par, s, at, head, tail)

            @pl.when(jnp.logical_not(own))
            def _():
                blend(t, l, par, s, at, head_in, tail_in)

            if after is not None:
                after(s)
            return inner

        lax.fori_loop(0, half, one, 0)

    def pass_on(t, l, par):
        def choose(peer):
            for u in range(per // 2):
                one = order[l + 1, peer * per + 2 * u]
                two = order[l + 1, peer * per + 2 * u + 1]
                send[t, 1 - par, peer, u] = jnp.where(first_slot, mixed[t, 0, one], mixed[t, 1, two])

        hand_out(t, 1 - par, choose)

    pairs(0, col, head, tail)
    weights_here(0)
    pairs(0, 1 - col, head_in, tail_in)
    pass_on(0, 0, 0)
    pairs(1, col, head, tail)
    pairs(1, 1 - col, head_in, tail_in)
    pass_on(1, 0, 0)

    def level(l, carry):
        par = lax.rem(l, 2)
        weights_here(l)
        for t in range(2):
            combine(t, l, par)
            sent(t, 1 - par)
            pass_on(t, l, par)
        return carry

    lax.fori_loop(1, levels - 1, level, 0)

    reach = leafwise.shape[1]

    def rows(s):
        for b in [t * per + q for t in (s, s + half) for q in range(per)]:
            base = lax.div(row_start[b], ROWS)
            window = [flipped[base + i] for i in range(reach // ROWS)]
            values = jnp.where(first_slot, mixed[0, 0, b], mixed[1, 1, b])
            pair = jnp.concatenate([values, turn(values)], axis=0)
            leafwise[b] = jnp.dot(
                jnp.concatenate(window, axis=0), pair, preferred_element_type=jnp.float32
            ).astype(bf16)

    last = (levels - 1) % 2
    weights_here(levels - 1)
    combine(0, levels - 1, last)
    combine(1, levels - 1, last, rows)
    for t in range(2):
        sent(t, 1 - last)
        sent(t, last)
    for l in range(levels):
        for copy in weight_copies(l):
            copy.wait_send()


def rows_kernel(sizes, leafwise, out_hbm, out, sem):
    blocks, reach, _ = leafwise.shape
    points = out_hbm.shape[0]
    parts = sem.shape[0]
    chunk = points // parts
    group = 8
    row = lax.broadcasted_iota(jnp.int32, (ROWS, LANES), 0)

    def part(c):
        at = pl.ds(pl.multiple_of(c * chunk, chunk), chunk)
        return pltpu.make_async_copy(out.at[at], out_hbm.at[at], sem.at[c])

    def leaves(g, begin):
        start = begin
        for i in range(group):
            b = g * group + i
            base = pl.multiple_of(start // ROWS * ROWS, ROWS)
            before = out[pl.ds(base, ROWS), :]
            top = jnp.where(row < start - base, before, leafwise[b, pl.ds(0, ROWS), :])
            out[pl.ds(base, ROWS), :] = top
            out[pl.ds(base + ROWS, reach - ROWS), :] = leafwise[b, pl.ds(ROWS, reach - ROWS), :]
            start = start + sizes[0, b]

        @pl.when(start // chunk > begin // chunk)
        def _():
            part(begin // chunk).start()

        return start

    lax.fori_loop(0, blocks // group, leaves, jnp.int32(0))
    for c in range(parts):
        part(c).wait()


def local(
    n, signal, col_factor, row_factor, level_factor, col_leaf_sizes, row_leaf_sizes, level_order
):
    levels, _, halves, depth, rank, width = level_factor.shape
    blocks = col_leaf_sizes.shape[1]
    points, columns = signal.shape
    per = blocks // n
    bf16 = jnp.bfloat16
    smem = pl.BlockSpec(memory_space=pltpu.SMEM)
    vmem = pl.BlockSpec(memory_space=pltpu.VMEM)
    hbm = pl.BlockSpec(memory_space=pltpu.HBM)
    reach = LANES + ROWS
    factors = level_factor.reshape(levels, halves, depth, rank, width)
    leafwise = pl.pallas_call(
        functools.partial(main_kernel, n),
        out_shape=pltpu.VMEM((blocks, reach, columns), bf16),
        in_specs=[hbm] * 7,
        out_specs=vmem,
        scratch_shapes=[
            pltpu.VMEM((points // LANES, LANES, columns), bf16),
            pltpu.VMEM((points // LANES, 2 * rank, LANES), bf16),
            pltpu.VMEM((2 * rank, points), bf16),
            pltpu.VMEM(((points + reach) // ROWS, ROWS, 2 * rank), bf16),
            pltpu.VMEM((levels, halves, depth, rank, LANES), bf16),
            pltpu.VMEM((levels, depth, rank, LANES), bf16),
            pltpu.VMEM((levels, halves, depth, rank, LANES), bf16),
            pltpu.VMEM((levels, depth, rank, LANES), bf16),
            pltpu.VMEM((levels, halves, depth, rank, width - LANES), bf16),
            pltpu.VMEM((2, 2, blocks, rank, columns), bf16),
            pltpu.VMEM((2, 2, n, per // 2, rank, columns), bf16),
            pltpu.VMEM((2, 2, n, per // 2, rank, columns), bf16),
            pltpu.SMEM((1, blocks), jnp.int32),
            pltpu.SMEM((1, blocks), jnp.int32),
            pltpu.SMEM((levels, blocks), jnp.int32),
            pltpu.SMEM((blocks,), jnp.int32),
            pltpu.SMEM((blocks,), jnp.int32),
            pltpu.SemaphoreType.DMA((levels + 1, 3)),
            pltpu.SemaphoreType.DMA((points // LANES,)),
            pltpu.SemaphoreType.DMA((3,)),
            pltpu.SemaphoreType.DMA((levels, 2)),
            pltpu.SemaphoreType.DMA((levels, 2)),
            pltpu.SemaphoreType.DMA((2, 2, n)),
            pltpu.SemaphoreType.DMA((2, 2, n)),
        ],
        compiler_params=pltpu.CompilerParams(
            collective_id=0, has_side_effects=True, vmem_limit_bytes=58000000
        ),
        name="levels",
    )(
        signal.reshape(points // LANES, LANES, columns), col_factor, row_factor, factors, col_leaf_sizes, row_leaf_sizes,
        level_order.reshape(levels, blocks),
    )
    return pl.pallas_call(
        rows_kernel,
        out_shape=jax.ShapeDtypeStruct((points, columns), bf16),
        in_specs=[smem, vmem],
        out_specs=hbm,
        scratch_shapes=[
            pltpu.VMEM((points + reach, columns), bf16),
            pltpu.SemaphoreType.DMA((points // (8 * LANES),)),
        ],
        compiler_params=pltpu.CompilerParams(vmem_limit_bytes=16 << 20),
        name="rows",
    )(row_leaf_sizes, leafwise)


def solution(mesh):
    in_specs = (
        P("blk", "rhs"),
        P(None, "blk"),
        P(None, "blk"),
        P(None, "blk", None, "rhs", None, None),
        P("blk", None),
        P("blk", None),
        P(None, "blk", None),
    )
    return jax.shard_map(
        functools.partial(local, mesh.shape["blk"]),
        mesh=mesh, in_specs=in_specs, out_specs=P("blk", "rhs"), check_vma=False,
    )
```

```python
import functools

import jax
import jax.numpy as jnp
from jax import lax
from jax.experimental import pallas as pl
from jax.experimental.pallas import tpu as pltpu
from jax.sharding import PartitionSpec as P

LANES = 128
ROWS = 16
MESH = pl.DeviceIdType.MESH


def turn(values):
    half = values.shape[-1] // 2
    return jnp.concatenate([-values[:, half:], values[:, :half]], axis=1)


def main_kernel(
    n, sig_hbm, cf_hbm, rf_hbm, lf_hbm, col_sizes_hbm, row_sizes_hbm, order_hbm, leafwise,
    sig, cf, rf, flipped, head, tail, head_in, tail_in, loose, coef, send, arr,
    col_sizes, row_sizes, order, col_start, row_start,
    load_sem, cf_sem, small_sem, w_send, w_recv, a_send, a_recv,
):
    levels, _, depth, rank, _ = head.shape
    width = LANES + loose.shape[-1]
    blocks = coef.shape[0]
    chunks = sig.shape[0]
    per = blocks // n
    half = n // 2
    sources = n // 4
    me = lax.axis_index("blk")
    col = lax.axis_index("rhs")
    side = me // half
    place = lax.rem(me, half)
    bf16 = jnp.bfloat16

    smalls = [
        pltpu.make_async_copy(col_sizes_hbm, col_sizes, small_sem.at[0]),
        pltpu.make_async_copy(order_hbm, order, small_sem.at[1]),
        pltpu.make_async_copy(row_sizes_hbm, row_sizes, small_sem.at[2]),
    ]
    load_sig = pltpu.make_async_copy(sig_hbm, sig, load_sem.at[levels, 0])

    def load_cf(c):
        at = pl.ds(pl.multiple_of(c * LANES, LANES), LANES)
        return pltpu.make_async_copy(cf_hbm.at[:, at], cf.at[c], cf_sem)

    load_rf = pltpu.make_async_copy(rf_hbm, rf, load_sem.at[levels, 2])

    def loads(l):
        return (
            pltpu.make_async_copy(
                lf_hbm.at[l, :, :, :, pl.ds(0, LANES)], head.at[l], load_sem.at[l, 0]
            ),
            pltpu.make_async_copy(
                lf_hbm.at[l, :, :, :, pl.ds(LANES, width - LANES)], loose.at[l], load_sem.at[l, 1]
            ),
        )

    for copy in smalls:
        copy.start()
    load_sig.start()

    def start_cf(c, carry):
        load_cf(c).start()
        return carry

    lax.fori_loop(0, chunks, start_cf, 0)

    barrier = pltpu.get_barrier_semaphore()

    def greet(k, carry):
        peer = lax.rem(me + k, n)
        pl.semaphore_signal(barrier, inc=1, device_id=(peer, col), device_id_type=MESH)
        return carry

    lax.fori_loop(1, n, greet, 0)
    pl.semaphore_signal(barrier, inc=1, device_id=(me, 1 - col), device_id_type=MESH)

    for copy in smalls:
        copy.wait()

    def add_up(b, carry):
        first, last = carry
        col_start[b] = first
        row_start[b] = last
        return first + col_sizes[0, b], last + row_sizes[0, b]

    lax.fori_loop(0, blocks, add_up, (jnp.int32(0), jnp.int32(0)), unroll=8)

    def weight_copies(l):
        return [
            pltpu.make_async_remote_copy(
                src_ref=ref.at[l],
                dst_ref=into.at[l],
                send_sem=w_send.at[l, at],
                recv_sem=w_recv.at[l, at],
                device_id=(me, 1 - col),
                device_id_type=MESH,
            )
            for at, (ref, into) in enumerate(((head, head_in), (tail, tail_in)))
        ]

    def pack(l):
        def one(i, carry):
            tail[l, i] = jnp.concatenate([loose[l, 0, i], loose[l, 1, i]], axis=1)
            return carry

        lax.fori_loop(0, depth, one, 0, unroll=4)

    def block_copy(par, peer):
        return pltpu.make_async_remote_copy(
            src_ref=send.at[par, peer],
            dst_ref=arr.at[par, me],
            send_sem=a_send.at[par],
            recv_sem=a_recv.at[par, me],
            device_id=(peer, col),
            device_id_type=MESH,
        )

    def arrival(par, source):
        return pltpu.make_async_remote_copy(
            src_ref=send.at[par, source],
            dst_ref=arr.at[par, source],
            send_sem=a_send.at[par],
            recv_sem=a_recv.at[par, source],
            device_id=(source, col),
            device_id_type=MESH,
        )

    def across(k):
        return (1 - side) * half + lax.rem(place + k, half)

    def beside(k):
        return side * half + lax.rem(place + k, half)

    def hand_out(par, choose):
        def one(k, inner):
            choose(across(k))
            block_copy(par, across(k)).start()

            @pl.when(k > 0)
            def _():
                choose(beside(k))
                block_copy(par, beside(k)).start()

            return inner

        lax.fori_loop(0, half, one, 0)
        choose(me)
        pltpu.make_async_copy(send.at[par, me], arr.at[par, me], a_recv.at[par, me]).start()

    def sent(par):
        gone = send.at[par, pl.ds(0, n - 1)]
        pltpu.make_async_copy(gone, gone, a_send.at[par]).wait()

    window = 2 * LANES
    lane = lax.broadcasted_iota(jnp.int32, (1, window), 1)

    def leaves(peer):
        for q in range(per):
            b = order[0, peer * per + q]
            start = col_start[b]
            end = start + col_sizes[0, b]
            c = jnp.minimum(lax.div(start, LANES), chunks - 2)
            base = c * LANES
            inside = jnp.logical_and(lane >= start - base, lane < end - base)
            keep = jnp.where(inside, 1.0, 0.0).astype(bf16)
            weights = jnp.concatenate([cf[c], cf[c + 1]], axis=1) * keep
            values = jnp.concatenate([sig[c], sig[c + 1]], axis=0)
            sums = jnp.dot(weights, values, preferred_element_type=jnp.float32)
            send[0, peer, q] = (sums[:rank] + turn(sums[rank:])).astype(bf16)

    load_sig.wait()

    pltpu.make_async_copy(cf, cf, cf_sem).wait()
    for l in range(levels):
        for copy in loads(l):
            copy.start()
    load_rf.start()
    pl.semaphore_wait(barrier, n)
    loads(0)[0].wait()
    weight_copies(0)[0].start()
    hand_out(0, leaves)

    for l in range(levels):
        for copy in loads(l)[l == 0:]:
            copy.wait()
        pack(l)
        for copy in weight_copies(l)[l == 0:]:
            copy.start()
    load_rf.wait()

    def flip(c, inner):
        at = pl.ds(pl.multiple_of(c * LANES, LANES), LANES)
        rows = LANES // ROWS
        flipped[pl.ds(c * rows, rows)] = rf[:, at].T.reshape(rows, ROWS, 2 * rank)
        return inner

    lax.fori_loop(0, chunks, flip, 0, unroll=4)

    blank = jnp.zeros((2 * LANES - width, LANES), bf16)

    def blend(l, par, s, at, first, second):
        arrival(par, s).wait_recv()
        arrival(par, s + half).wait_recv()
        for q in range(per):
            i = at * per + q
            x = arr[par, s, q]
            y = arr[par, s + half, q]
            jx = turn(x)
            jy = turn(y)
            rest = second[l, i]
            upper = jnp.concatenate([first[l, 0, i], rest], axis=1)
            lower = jnp.concatenate([first[l, 1, i], rest], axis=1)
            cut = LANES - 2 * rank
            over = jnp.concatenate([x, jx, y, jy, blank], axis=0)
            under = jnp.concatenate([y, jy, x[:cut], blank, x[cut:], jx], axis=0)
            coef[s * per + q] = jnp.dot(
                upper, over, preferred_element_type=jnp.float32
            ).astype(bf16)
            coef[(s + half) * per + q] = jnp.dot(
                lower, under, preferred_element_type=jnp.float32
            ).astype(bf16)

    def weights_here(l):
        for copy in weight_copies(l):
            copy.wait_recv()

    def combine_first(par):
        def pairs(owner, first, second):
            def one(k, inner):
                at = lax.rem(place + sources - k, sources)
                blend(0, par, owner * sources + at, at, first, second)
                return inner

            lax.fori_loop(0, sources, one, 0)

        pairs(col, head, tail)
        weights_here(0)
        pairs(1 - col, head_in, tail_in)

    def combine(l, par, after=None):
        weights_here(l)

        def one(k, inner):
            s = lax.rem(place + half - k, half)
            at = lax.rem(s, sources)
            own = s // sources == col

            @pl.when(own)
            def _():
                blend(l, par, s, at, head, tail)

            @pl.when(jnp.logical_not(own))
            def _():
                blend(l, par, s, at, head_in, tail_in)

            if after is not None:
                after(s)
            return inner

        lax.fori_loop(0, half, one, 0)

    def pass_on(l, par):
        def choose(peer):
            for q in range(per):
                send[1 - par, peer, q] = coef[order[l + 1, peer * per + q]]

        hand_out(1 - par, choose)

    combine_first(0)
    pass_on(0, 0)

    def level(l, carry):
        par = lax.rem(l, 2)
        combine(l, par)
        sent(1 - par)
        pass_on(l, par)
        return carry

    lax.fori_loop(1, levels - 1, level, 0)

    reach = leafwise.shape[1]

    def rows(s):
        for b in [t * per + q for t in (s, s + half) for q in range(per)]:
            base = lax.div(row_start[b], ROWS)
            window = [flipped[base + i] for i in range(reach // ROWS)]
            values = coef[b]
            pair = jnp.concatenate([values, turn(values)], axis=0)
            leafwise[b] = jnp.dot(
                jnp.concatenate(window, axis=0), pair, preferred_element_type=jnp.float32
            ).astype(bf16)

    last = (levels - 1) % 2
    combine(levels - 1, last, rows)
    sent(1 - last)
    sent(last)
    for l in range(levels):
        for copy in weight_copies(l):
            copy.wait_send()


def rows_kernel(sizes, leafwise, out_hbm, out, sem):
    blocks, reach, _ = leafwise.shape
    points = out_hbm.shape[0]
    parts = sem.shape[0]
    chunk = points // parts
    group = 8
    row = lax.broadcasted_iota(jnp.int32, (ROWS, LANES), 0)

    def part(c):
        at = pl.ds(pl.multiple_of(c * chunk, chunk), chunk)
        return pltpu.make_async_copy(out.at[at], out_hbm.at[at], sem.at[c])

    def leaves(g, begin):
        start = begin
        for i in range(group):
            b = g * group + i
            base = pl.multiple_of(start // ROWS * ROWS, ROWS)
            before = out[pl.ds(base, ROWS), :]
            top = jnp.where(row < start - base, before, leafwise[b, pl.ds(0, ROWS), :])
            out[pl.ds(base, ROWS), :] = top
            out[pl.ds(base + ROWS, reach - ROWS), :] = leafwise[b, pl.ds(ROWS, reach - ROWS), :]
            start = start + sizes[0, b]

        @pl.when(start // chunk > begin // chunk)
        def _():
            part(begin // chunk).start()

        return start

    lax.fori_loop(0, blocks // group, leaves, jnp.int32(0))
    for c in range(parts):
        part(c).wait()


def local(
    n, signal, col_factor, row_factor, level_factor, col_leaf_sizes, row_leaf_sizes, level_order
):
    levels, _, halves, depth, rank, width = level_factor.shape
    blocks = col_leaf_sizes.shape[1]
    points, columns = signal.shape
    per = blocks // n
    bf16 = jnp.bfloat16
    smem = pl.BlockSpec(memory_space=pltpu.SMEM)
    vmem = pl.BlockSpec(memory_space=pltpu.VMEM)
    hbm = pl.BlockSpec(memory_space=pltpu.HBM)
    reach = LANES + ROWS
    factors = level_factor.reshape(levels, halves, depth, rank, width)
    leafwise = pl.pallas_call(
        functools.partial(main_kernel, n),
        out_shape=pltpu.VMEM((blocks, reach, columns), bf16),
        in_specs=[hbm] * 7,
        out_specs=vmem,
        scratch_shapes=[
            pltpu.VMEM((points // LANES, LANES, columns), bf16),
            pltpu.VMEM((points // LANES, 2 * rank, LANES), bf16),
            pltpu.VMEM((2 * rank, points), bf16),
            pltpu.VMEM(((points + reach) // ROWS, ROWS, 2 * rank), bf16),
            pltpu.VMEM((levels, halves, depth, rank, LANES), bf16),
            pltpu.VMEM((levels, depth, rank, LANES), bf16),
            pltpu.VMEM((levels, halves, depth, rank, LANES), bf16),
            pltpu.VMEM((levels, depth, rank, LANES), bf16),
            pltpu.VMEM((levels, halves, depth, rank, width - LANES), bf16),
            pltpu.VMEM((blocks, rank, columns), bf16),
            pltpu.VMEM((2, n, per, rank, columns), bf16),
            pltpu.VMEM((2, n, per, rank, columns), bf16),
            pltpu.SMEM((1, blocks), jnp.int32),
            pltpu.SMEM((1, blocks), jnp.int32),
            pltpu.SMEM((levels, blocks), jnp.int32),
            pltpu.SMEM((blocks,), jnp.int32),
            pltpu.SMEM((blocks,), jnp.int32),
            pltpu.SemaphoreType.DMA((levels + 1, 3)),
            pltpu.SemaphoreType.DMA(()),
            pltpu.SemaphoreType.DMA((3,)),
            pltpu.SemaphoreType.DMA((levels, 2)),
            pltpu.SemaphoreType.DMA((levels, 2)),
            pltpu.SemaphoreType.DMA((2,)),
            pltpu.SemaphoreType.DMA((2, n)),
        ],
        compiler_params=pltpu.CompilerParams(
            collective_id=0, has_side_effects=True, vmem_limit_bytes=58000000
        ),
        name="levels",
    )(
        signal.reshape(points // LANES, LANES, columns), col_factor, row_factor, factors, col_leaf_sizes, row_leaf_sizes,
        level_order.reshape(levels, blocks),
    )
    return pl.pallas_call(
        rows_kernel,
        out_shape=jax.ShapeDtypeStruct((points, columns), bf16),
        in_specs=[smem, vmem],
        out_specs=hbm,
        scratch_shapes=[
            pltpu.VMEM((points + reach, columns), bf16),
            pltpu.SemaphoreType.DMA((points // (8 * LANES),)),
        ],
        compiler_params=pltpu.CompilerParams(vmem_limit_bytes=16 << 20),
        name="rows",
    )(row_leaf_sizes, leafwise)


def solution(mesh):
    in_specs = (
        P("blk", "rhs"),
        P(None, "blk"),
        P(None, "blk"),
        P(None, "blk", None, "rhs", None, None),
        P("blk", None),
        P("blk", None),
        P(None, "blk", None),
    )
    return jax.shard_map(
        functools.partial(local, mesh.shape["blk"]),
        mesh=mesh, in_specs=in_specs, out_specs=P("blk", "rhs"), check_vma=False,
    )
```

```python
import functools

import jax
import jax.numpy as jnp
from jax import lax
from jax.experimental import pallas as pl
from jax.experimental.pallas import tpu as pltpu
from jax.sharding import PartitionSpec as P

LANES = 128
ROWS = 16
MESH = pl.DeviceIdType.MESH


def turn(values):
    half = values.shape[-1] // 2
    return jnp.concatenate([-values[:, half:], values[:, :half]], axis=1)


def main_kernel(
    n, sig_hbm, cf_hbm, rf_hbm, lf_hbm, col_sizes_hbm, row_sizes_hbm, order_hbm, leafwise,
    sig, cf, rf, flipped, head, tail, head_in, tail_in, loose, coef, send, arr,
    col_sizes, row_sizes, order, col_start, row_start,
    load_sem, cf_sem, small_sem, w_send, w_recv, a_send, a_recv,
):
    levels, _, depth, rank, _ = head.shape
    width = LANES + loose.shape[-1]
    blocks = coef.shape[0]
    chunks = sig.shape[0]
    per = blocks // n
    half = n // 2
    sources = n // 4
    me = lax.axis_index("blk")
    col = lax.axis_index("rhs")
    side = me // half
    place = lax.rem(me, half)
    bf16 = jnp.bfloat16

    smalls = [
        pltpu.make_async_copy(col_sizes_hbm, col_sizes, small_sem.at[0]),
        pltpu.make_async_copy(order_hbm, order, small_sem.at[1]),
        pltpu.make_async_copy(row_sizes_hbm, row_sizes, small_sem.at[2]),
    ]
    load_sig = pltpu.make_async_copy(sig_hbm, sig, load_sem.at[0])

    def load_cf(c):
        at = pl.ds(pl.multiple_of(c * LANES, LANES), LANES)
        return pltpu.make_async_copy(cf_hbm.at[:, at], cf.at[c], cf_sem)

    load_rf = pltpu.make_async_copy(rf_hbm, rf, load_sem.at[1])

    tops = pl.ds(0, LANES)
    load_head = pltpu.make_async_copy(
        lf_hbm.at[0, :, :, :, tops], head.at[0], load_sem.at[2]
    )
    later = pl.ds(1, levels - 1)
    load_heads = pltpu.make_async_copy(
        lf_hbm.at[later, :, :, :, tops], head.at[later], load_sem.at[3]
    )
    load_loose = pltpu.make_async_copy(
        lf_hbm.at[:, :, :, :, pl.ds(LANES, width - LANES)], loose, load_sem.at[4]
    )

    barrier = pltpu.get_barrier_semaphore()

    def greet(k, carry):
        peer = lax.rem(me + k, n)
        pl.semaphore_signal(barrier, inc=1, device_id=(peer, col), device_id_type=MESH)
        return carry

    lax.fori_loop(1, n, greet, 0)
    pl.semaphore_signal(barrier, inc=1, device_id=(me, 1 - col), device_id_type=MESH)

    for copy in smalls:
        copy.start()
    load_sig.start()

    def start_cf(c, carry):
        load_cf(c).start()
        return carry

    lax.fori_loop(0, chunks, start_cf, 0)

    for copy in smalls:
        copy.wait()

    def add_up(b, carry):
        first, last = carry
        col_start[b] = first
        row_start[b] = last
        return first + col_sizes[0, b], last + row_sizes[0, b]

    lax.fori_loop(0, blocks, add_up, (jnp.int32(0), jnp.int32(0)), unroll=8)

    def weight_copy(l, at, ref, into):
        return pltpu.make_async_remote_copy(
            src_ref=ref.at[l],
            dst_ref=into.at[l],
            send_sem=w_send.at[at],
            recv_sem=w_recv.at[l, at],
            device_id=(me, 1 - col),
            device_id_type=MESH,
        )

    def head_copy(l):
        return weight_copy(l, 0, head, head_in)

    def tail_copy(l):
        return weight_copy(l, 1, tail, tail_in)

    def pack(l):
        def one(i, carry):
            tail[l, i] = jnp.concatenate([loose[l, 0, i], loose[l, 1, i]], axis=1)
            return carry

        lax.fori_loop(0, depth, one, 0, unroll=4)

    def block_copy(par, peer):
        return pltpu.make_async_remote_copy(
            src_ref=send.at[par, peer],
            dst_ref=arr.at[par, me],
            send_sem=a_send.at[par],
            recv_sem=a_recv.at[par, me],
            device_id=(peer, col),
            device_id_type=MESH,
        )

    def arrival(par, source):
        return pltpu.make_async_remote_copy(
            src_ref=send.at[par, source],
            dst_ref=arr.at[par, source],
            send_sem=a_send.at[par],
            recv_sem=a_recv.at[par, source],
            device_id=(source, col),
            device_id_type=MESH,
        )

    def across(k):
        return (1 - side) * half + lax.rem(place + k, half)

    def beside(k):
        return side * half + lax.rem(place + k, half)

    def hand_out(par, choose):
        def one(k, inner):
            @pl.when(k > 0)
            def _():
                choose(beside(k))
                block_copy(par, beside(k)).start()

            choose(across(k))
            block_copy(par, across(k)).start()
            return inner

        lax.fori_loop(0, half, one, 0)
        choose(me)
        pltpu.make_async_copy(send.at[par, me], arr.at[par, me], a_recv.at[par, me]).start()

    def sent(par):
        gone = send.at[par, pl.ds(0, n - 1)]
        pltpu.make_async_copy(gone, gone, a_send.at[par]).wait()

    window = 2 * LANES
    lane = lax.broadcasted_iota(jnp.int32, (1, window), 1)

    def leaves(peer):
        for q in range(per):
            b = order[0, peer * per + q]
            start = col_start[b]
            end = start + col_sizes[0, b]
            c = jnp.minimum(lax.div(start, LANES), chunks - 2)
            base = c * LANES
            inside = jnp.logical_and(lane >= start - base, lane < end - base)
            keep = jnp.where(inside, 1.0, 0.0).astype(bf16)
            weights = jnp.concatenate([cf[c], cf[c + 1]], axis=1) * keep
            values = jnp.concatenate([sig[c], sig[c + 1]], axis=0)
            sums = jnp.dot(weights, values, preferred_element_type=jnp.float32)
            send[0, peer, q] = (sums[:rank] + turn(sums[rank:])).astype(bf16)

    load_sig.wait()

    pltpu.make_async_copy(cf, cf, cf_sem).wait()
    load_head.start()
    load_loose.start()
    load_heads.start()
    load_rf.start()
    pl.semaphore_wait(barrier, n)
    load_head.wait()
    head_copy(0).start()
    hand_out(0, leaves)

    load_loose.wait()
    pack(0)
    tail_copy(0).start()
    load_heads.wait()
    for l in range(1, levels):
        head_copy(l).start()
        pack(l)
        tail_copy(l).start()
    load_rf.wait()

    def flip(c, inner):
        at = pl.ds(pl.multiple_of(c * LANES, LANES), LANES)
        rows = LANES // ROWS
        flipped[pl.ds(c * rows, rows)] = rf[:, at].T.reshape(rows, ROWS, 2 * rank)
        return inner

    lax.fori_loop(0, chunks, flip, 0, unroll=4)

    blank = jnp.zeros((2 * LANES - width, LANES), bf16)

    def blend(l, par, s, at, first, second):
        arrival(par, s).wait_recv()
        arrival(par, s + half).wait_recv()
        for q in range(per):
            i = at * per + q
            x = arr[par, s, q]
            y = arr[par, s + half, q]
            jx = turn(x)
            jy = turn(y)
            rest = second[l, i]
            upper = jnp.concatenate([first[l, 0, i], rest], axis=1)
            lower = jnp.concatenate([first[l, 1, i], rest], axis=1)
            cut = LANES - 2 * rank
            over = jnp.concatenate([x, jx, y, jy, blank], axis=0)
            under = jnp.concatenate([y, jy, x[:cut], blank, x[cut:], jx], axis=0)
            coef[s * per + q] = jnp.dot(
                upper, over, preferred_element_type=jnp.float32
            ).astype(bf16)
            coef[(s + half) * per + q] = jnp.dot(
                lower, under, preferred_element_type=jnp.float32
            ).astype(bf16)

    def weights_here(l):
        head_copy(l).wait_recv()
        tail_copy(l).wait_recv()

    def combine(l, par, after=None):
        weights_here(l)

        def one(k, inner):
            s = lax.rem(place + half - k, half)
            at = lax.rem(s, sources)
            own = s // sources == col

            @pl.when(own)
            def _():
                blend(l, par, s, at, head, tail)

            @pl.when(jnp.logical_not(own))
            def _():
                blend(l, par, s, at, head_in, tail_in)

            if after is not None:
                after(s)
            return inner

        lax.fori_loop(0, half, one, 0)

    def pass_on(l, par):
        def choose(peer):
            for q in range(per):
                send[1 - par, peer, q] = coef[order[l + 1, peer * per + q]]

        hand_out(1 - par, choose)

    def level(l, carry):
        par = lax.rem(l, 2)
        combine(l, par)

        @pl.when(l > 0)
        def _():
            sent(1 - par)

        pass_on(l, par)
        return carry

    lax.fori_loop(0, levels - 1, level, 0)

    reach = leafwise.shape[1]

    def rows(s):
        for b in [t * per + q for t in (s, s + half) for q in range(per)]:
            base = lax.div(row_start[b], ROWS)
            window = [flipped[base + i] for i in range(reach // ROWS)]
            values = coef[b]
            pair = jnp.concatenate([values, turn(values)], axis=0)
            leafwise[b] = jnp.dot(
                jnp.concatenate(window, axis=0), pair, preferred_element_type=jnp.float32
            ).astype(bf16)

    last = (levels - 1) % 2
    combine(levels - 1, last, rows)
    sent(1 - last)
    sent(last)
    pltpu.make_async_copy(head, head, w_send.at[0]).wait()
    pltpu.make_async_copy(tail, tail, w_send.at[1]).wait()


def rows_kernel(sizes, leafwise, out_hbm, out, sem):
    blocks, reach, _ = leafwise.shape
    points = out_hbm.shape[0]
    parts = sem.shape[0]
    chunk = points // parts
    group = 8
    row = lax.broadcasted_iota(jnp.int32, (ROWS, LANES), 0)

    def part(c):
        at = pl.ds(pl.multiple_of(c * chunk, chunk), chunk)
        return pltpu.make_async_copy(out.at[at], out_hbm.at[at], sem.at[c])

    def leaves(g, begin):
        start = begin
        for i in range(group):
            b = g * group + i
            base = pl.multiple_of(start // ROWS * ROWS, ROWS)
            before = out[pl.ds(base, ROWS), :]
            top = jnp.where(row < start - base, before, leafwise[b, pl.ds(0, ROWS), :])
            out[pl.ds(base, ROWS), :] = top
            out[pl.ds(base + ROWS, reach - ROWS), :] = leafwise[b, pl.ds(ROWS, reach - ROWS), :]
            start = start + sizes[0, b]

        @pl.when(start // chunk > begin // chunk)
        def _():
            part(begin // chunk).start()

        return start

    lax.fori_loop(0, blocks // group, leaves, jnp.int32(0))
    for c in range(parts):
        part(c).wait()


def local(
    n, signal, col_factor, row_factor, level_factor, col_leaf_sizes, row_leaf_sizes, level_order
):
    levels, _, halves, depth, rank, width = level_factor.shape
    blocks = col_leaf_sizes.shape[1]
    points, columns = signal.shape
    per = blocks // n
    bf16 = jnp.bfloat16
    smem = pl.BlockSpec(memory_space=pltpu.SMEM)
    vmem = pl.BlockSpec(memory_space=pltpu.VMEM)
    hbm = pl.BlockSpec(memory_space=pltpu.HBM)
    reach = LANES + ROWS
    factors = level_factor.reshape(levels, halves, depth, rank, width)
    leafwise = pl.pallas_call(
        functools.partial(main_kernel, n),
        out_shape=pltpu.VMEM((blocks, reach, columns), bf16),
        in_specs=[hbm] * 7,
        out_specs=vmem,
        scratch_shapes=[
            pltpu.VMEM((points // LANES, LANES, columns), bf16),
            pltpu.VMEM((points // LANES, 2 * rank, LANES), bf16),
            pltpu.VMEM((2 * rank, points), bf16),
            pltpu.VMEM(((points + reach) // ROWS, ROWS, 2 * rank), bf16),
            pltpu.VMEM((levels, halves, depth, rank, LANES), bf16),
            pltpu.VMEM((levels, depth, rank, LANES), bf16),
            pltpu.VMEM((levels, halves, depth, rank, LANES), bf16),
            pltpu.VMEM((levels, depth, rank, LANES), bf16),
            pltpu.VMEM((levels, halves, depth, rank, width - LANES), bf16),
            pltpu.VMEM((blocks, rank, columns), bf16),
            pltpu.VMEM((2, n, per, rank, columns), bf16),
            pltpu.VMEM((2, n, per, rank, columns), bf16),
            pltpu.SMEM((1, blocks), jnp.int32),
            pltpu.SMEM((1, blocks), jnp.int32),
            pltpu.SMEM((levels, blocks), jnp.int32),
            pltpu.SMEM((blocks,), jnp.int32),
            pltpu.SMEM((blocks,), jnp.int32),
            pltpu.SemaphoreType.DMA((5,)),
            pltpu.SemaphoreType.DMA(()),
            pltpu.SemaphoreType.DMA((3,)),
            pltpu.SemaphoreType.DMA((2,)),
            pltpu.SemaphoreType.DMA((levels, 2)),
            pltpu.SemaphoreType.DMA((2,)),
            pltpu.SemaphoreType.DMA((2, n)),
        ],
        compiler_params=pltpu.CompilerParams(
            collective_id=0, has_side_effects=True, vmem_limit_bytes=58000000
        ),
        name="levels",
    )(
        signal.reshape(points // LANES, LANES, columns), col_factor, row_factor, factors, col_leaf_sizes, row_leaf_sizes,
        level_order.reshape(levels, blocks),
    )
    return pl.pallas_call(
        rows_kernel,
        out_shape=jax.ShapeDtypeStruct((points, columns), bf16),
        in_specs=[smem, vmem],
        out_specs=hbm,
        scratch_shapes=[
            pltpu.VMEM((points + reach, columns), bf16),
            pltpu.SemaphoreType.DMA((points // (8 * LANES),)),
        ],
        compiler_params=pltpu.CompilerParams(vmem_limit_bytes=16 << 20),
        name="rows",
    )(row_leaf_sizes, leafwise)


def solution(mesh):
    in_specs = (
        P("blk", "rhs"),
        P(None, "blk"),
        P(None, "blk"),
        P(None, "blk", None, "rhs", None, None),
        P("blk", None),
        P("blk", None),
        P(None, "blk", None),
    )
    return jax.shard_map(
        functools.partial(local, mesh.shape["blk"]),
        mesh=mesh, in_specs=in_specs, out_specs=P("blk", "rhs"), check_vma=False,
    )
```

```python
import functools

import jax
import jax.numpy as jnp
from jax import lax
from jax.experimental import pallas as pl
from jax.experimental.pallas import tpu as pltpu
from jax.sharding import PartitionSpec as P

LANES = 128
ROWS = 16
MESH = pl.DeviceIdType.MESH


def turn(values):
    half = values.shape[-1] // 2
    return jnp.concatenate([-values[:, half:], values[:, :half]], axis=1)


def main_kernel(
    n, sig_hbm, cf_hbm, rf_hbm, lf_hbm, col_sizes_hbm, row_sizes_hbm, order_hbm, leafwise,
    sig, cf, rf, flipped, head, tail, head_in, tail_in, loose, coef, send, arr,
    col_sizes, row_sizes, order, col_start, row_start,
    load_sem, cf_sem, small_sem, w_send, w_recv, a_send, a_recv,
):
    levels, _, depth, rank, _ = head.shape
    width = LANES + loose.shape[-1]
    blocks = coef.shape[0]
    chunks = sig.shape[0]
    per = blocks // n
    half = n // 2
    sources = n // 4
    me = lax.axis_index("blk")
    col = lax.axis_index("rhs")
    side = me // half
    place = lax.rem(me, half)
    bf16 = jnp.bfloat16

    smalls = [
        pltpu.make_async_copy(col_sizes_hbm, col_sizes, small_sem.at[0]),
        pltpu.make_async_copy(order_hbm, order, small_sem.at[1]),
        pltpu.make_async_copy(row_sizes_hbm, row_sizes, small_sem.at[2]),
    ]
    load_sig = pltpu.make_async_copy(sig_hbm, sig, load_sem.at[0])

    def load_cf(c):
        at = pl.ds(pl.multiple_of(c * LANES, LANES), LANES)
        return pltpu.make_async_copy(cf_hbm.at[:, at], cf.at[c], cf_sem)

    load_rf = pltpu.make_async_copy(rf_hbm, rf, load_sem.at[1])

    tops = pl.ds(0, LANES)
    load_head = pltpu.make_async_copy(
        lf_hbm.at[0, :, :, :, tops], head.at[0], load_sem.at[2]
    )
    later = pl.ds(1, levels - 1)
    load_heads = pltpu.make_async_copy(
        lf_hbm.at[later, :, :, :, tops], head.at[later], load_sem.at[3]
    )
    load_loose = pltpu.make_async_copy(
        lf_hbm.at[:, :, :, :, pl.ds(LANES, width - LANES)], loose, load_sem.at[4]
    )

    barrier = pltpu.get_barrier_semaphore()

    def greet(k, carry):
        peer = lax.rem(me + k, n)
        pl.semaphore_signal(barrier, inc=1, device_id=(peer, col), device_id_type=MESH)
        return carry

    lax.fori_loop(1, n, greet, 0)
    pl.semaphore_signal(barrier, inc=1, device_id=(me, 1 - col), device_id_type=MESH)

    for copy in smalls:
        copy.start()
    load_sig.start()

    def start_cf(c, carry):
        load_cf(c).start()
        return carry

    lax.fori_loop(0, chunks, start_cf, 0)

    for copy in smalls:
        copy.wait()

    def add_up(b, carry):
        first, last = carry
        col_start[b] = first
        row_start[b] = last
        return first + col_sizes[0, b], last + row_sizes[0, b]

    lax.fori_loop(0, blocks, add_up, (jnp.int32(0), jnp.int32(0)), unroll=8)

    def weight_copy(l, at, ref, into):
        return pltpu.make_async_remote_copy(
            src_ref=ref.at[l],
            dst_ref=into.at[l],
            send_sem=w_send.at[at],
            recv_sem=w_recv.at[l, at],
            device_id=(me, 1 - col),
            device_id_type=MESH,
        )

    def head_copy(l):
        return weight_copy(l, 0, head, head_in)

    def tail_copy(l):
        return weight_copy(l, 1, tail, tail_in)

    def pack(l):
        def one(i, carry):
            tail[l, i] = jnp.concatenate([loose[l, 0, i], loose[l, 1, i]], axis=1)
            return carry

        lax.fori_loop(0, depth, one, 0, unroll=4)

    def block_copy(par, peer):
        return pltpu.make_async_remote_copy(
            src_ref=send.at[par, peer],
            dst_ref=arr.at[par, me],
            send_sem=a_send.at[par],
            recv_sem=a_recv.at[par, me],
            device_id=(peer, col),
            device_id_type=MESH,
        )

    def arrival(par, source):
        return pltpu.make_async_remote_copy(
            src_ref=send.at[par, source],
            dst_ref=arr.at[par, source],
            send_sem=a_send.at[par],
            recv_sem=a_recv.at[par, source],
            device_id=(source, col),
            device_id_type=MESH,
        )

    def across(k):
        return (1 - side) * half + lax.rem(place + k, half)

    def beside(k):
        return side * half + lax.rem(place + k, half)

    def hand_out(par, choose, chosen=0):
        def one(k, inner):
            @pl.when(k > 0)
            def _():
                choose(beside(k))
                block_copy(par, beside(k)).start()

            @pl.when(k >= chosen)
            def _():
                choose(across(k))

            block_copy(par, across(k)).start()
            return inner

        lax.fori_loop(0, half, one, 0)
        choose(me)
        pltpu.make_async_copy(send.at[par, me], arr.at[par, me], a_recv.at[par, me]).start()

    def sent(par):
        gone = send.at[par, pl.ds(0, n - 1)]
        pltpu.make_async_copy(gone, gone, a_send.at[par]).wait()

    window = 2 * LANES
    lane = lax.broadcasted_iota(jnp.int32, (1, window), 1)

    def leaves(peer):
        for q in range(per):
            b = order[0, peer * per + q]
            start = col_start[b]
            end = start + col_sizes[0, b]
            c = jnp.minimum(lax.div(start, LANES), chunks - 2)
            base = c * LANES
            inside = jnp.logical_and(lane >= start - base, lane < end - base)
            keep = jnp.where(inside, 1.0, 0.0).astype(bf16)
            weights = jnp.concatenate([cf[c], cf[c + 1]], axis=1) * keep
            values = jnp.concatenate([sig[c], sig[c + 1]], axis=0)
            sums = jnp.dot(weights, values, preferred_element_type=jnp.float32)
            send[0, peer, q] = (sums[:rank] + turn(sums[rank:])).astype(bf16)

    load_sig.wait()

    pltpu.make_async_copy(cf, cf, cf_sem).wait()
    load_head.start()
    load_loose.start()
    load_heads.start()
    load_rf.start()
    leaves(across(0))
    leaves(across(1))
    load_head.wait()
    pl.semaphore_wait(barrier, n)
    head_copy(0).start()
    hand_out(0, leaves, 2)

    load_loose.wait()
    pack(0)
    tail_copy(0).start()
    load_heads.wait()
    for l in range(1, levels):
        head_copy(l).start()
        pack(l)
        tail_copy(l).start()
    load_rf.wait()

    def flip(c, inner):
        at = pl.ds(pl.multiple_of(c * LANES, LANES), LANES)
        rows = LANES // ROWS
        flipped[pl.ds(c * rows, rows)] = rf[:, at].T.reshape(rows, ROWS, 2 * rank)
        return inner

    lax.fori_loop(0, chunks, flip, 0, unroll=4)

    blank = jnp.zeros((2 * LANES - width, LANES), bf16)

    def blend(l, par, s, at, first, second):
        arrival(par, s).wait_recv()
        arrival(par, s + half).wait_recv()
        for q in range(per):
            i = at * per + q
            x = arr[par, s, q]
            y = arr[par, s + half, q]
            jx = turn(x)
            jy = turn(y)
            rest = second[l, i]
            upper = jnp.concatenate([first[l, 0, i], rest], axis=1)
            lower = jnp.concatenate([first[l, 1, i], rest], axis=1)
            cut = LANES - 2 * rank
            over = jnp.concatenate([x, jx, y, jy, blank], axis=0)
            under = jnp.concatenate([y, jy, x[:cut], blank, x[cut:], jx], axis=0)
            coef[s * per + q] = jnp.dot(
                upper, over, preferred_element_type=jnp.float32
            ).astype(bf16)
            coef[(s + half) * per + q] = jnp.dot(
                lower, under, preferred_element_type=jnp.float32
            ).astype(bf16)

    def weights_here(l):
        head_copy(l).wait_recv()
        tail_copy(l).wait_recv()

    def combine(l, par, after=None):
        weights_here(l)

        def one(k, inner):
            s = lax.rem(place + half - k, half)
            at = lax.rem(s, sources)
            own = s // sources == col

            @pl.when(own)
            def _():
                blend(l, par, s, at, head, tail)

            @pl.when(jnp.logical_not(own))
            def _():
                blend(l, par, s, at, head_in, tail_in)

            if after is not None:
                after(s)
            return inner

        lax.fori_loop(0, half, one, 0)

    def pass_on(l, par):
        def choose(peer):
            for q in range(per):
                send[1 - par, peer, q] = coef[order[l + 1, peer * per + q]]

        hand_out(1 - par, choose)

    def level(l, carry):
        par = lax.rem(l, 2)
        combine(l, par)

        @pl.when(l > 0)
        def _():
            sent(1 - par)

        pass_on(l, par)
        return carry

    lax.fori_loop(0, levels - 1, level, 0)

    reach = leafwise.shape[1]

    def rows(s):
        for b in [t * per + q for t in (s, s + half) for q in range(per)]:
            base = lax.div(row_start[b], ROWS)
            window = [flipped[base + i] for i in range(reach // ROWS)]
            values = coef[b]
            pair = jnp.concatenate([values, turn(values)], axis=0)
            leafwise[b] = jnp.dot(
                jnp.concatenate(window, axis=0), pair, preferred_element_type=jnp.float32
            ).astype(bf16)

    last = (levels - 1) % 2
    combine(levels - 1, last, rows)
    sent(1 - last)
    sent(last)
    pltpu.make_async_copy(head, head, w_send.at[0]).wait()
    pltpu.make_async_copy(tail, tail, w_send.at[1]).wait()


def rows_kernel(sizes, leafwise, out_hbm, out, sem):
    blocks, reach, _ = leafwise.shape
    points = out_hbm.shape[0]
    parts = sem.shape[0]
    chunk = points // parts
    group = 8
    row = lax.broadcasted_iota(jnp.int32, (ROWS, LANES), 0)

    def part(c):
        at = pl.ds(pl.multiple_of(c * chunk, chunk), chunk)
        return pltpu.make_async_copy(out.at[at], out_hbm.at[at], sem.at[c])

    def leaves(g, begin):
        start = begin
        for i in range(group):
            b = g * group + i
            base = pl.multiple_of(start // ROWS * ROWS, ROWS)
            before = out[pl.ds(base, ROWS), :]
            top = jnp.where(row < start - base, before, leafwise[b, pl.ds(0, ROWS), :])
            out[pl.ds(base, ROWS), :] = top
            out[pl.ds(base + ROWS, reach - ROWS), :] = leafwise[b, pl.ds(ROWS, reach - ROWS), :]
            start = start + sizes[0, b]

        @pl.when(start // chunk > begin // chunk)
        def _():
            part(begin // chunk).start()

        return start

    lax.fori_loop(0, blocks // group, leaves, jnp.int32(0))
    for c in range(parts):
        part(c).wait()


def local(
    n, signal, col_factor, row_factor, level_factor, col_leaf_sizes, row_leaf_sizes, level_order
):
    levels, _, halves, depth, rank, width = level_factor.shape
    blocks = col_leaf_sizes.shape[1]
    points, columns = signal.shape
    per = blocks // n
    bf16 = jnp.bfloat16
    smem = pl.BlockSpec(memory_space=pltpu.SMEM)
    vmem = pl.BlockSpec(memory_space=pltpu.VMEM)
    hbm = pl.BlockSpec(memory_space=pltpu.HBM)
    reach = LANES + ROWS
    factors = level_factor.reshape(levels, halves, depth, rank, width)
    leafwise = pl.pallas_call(
        functools.partial(main_kernel, n),
        out_shape=pltpu.VMEM((blocks, reach, columns), bf16),
        in_specs=[hbm] * 7,
        out_specs=vmem,
        scratch_shapes=[
            pltpu.VMEM((points // LANES, LANES, columns), bf16),
            pltpu.VMEM((points // LANES, 2 * rank, LANES), bf16),
            pltpu.VMEM((2 * rank, points), bf16),
            pltpu.VMEM(((points + reach) // ROWS, ROWS, 2 * rank), bf16),
            pltpu.VMEM((levels, halves, depth, rank, LANES), bf16),
            pltpu.VMEM((levels, depth, rank, LANES), bf16),
            pltpu.VMEM((levels, halves, depth, rank, LANES), bf16),
            pltpu.VMEM((levels, depth, rank, LANES), bf16),
            pltpu.VMEM((levels, halves, depth, rank, width - LANES), bf16),
            pltpu.VMEM((blocks, rank, columns), bf16),
            pltpu.VMEM((2, n, per, rank, columns), bf16),
            pltpu.VMEM((2, n, per, rank, columns), bf16),
            pltpu.SMEM((1, blocks), jnp.int32),
            pltpu.SMEM((1, blocks), jnp.int32),
            pltpu.SMEM((levels, blocks), jnp.int32),
            pltpu.SMEM((blocks,), jnp.int32),
            pltpu.SMEM((blocks,), jnp.int32),
            pltpu.SemaphoreType.DMA((5,)),
            pltpu.SemaphoreType.DMA(()),
            pltpu.SemaphoreType.DMA((3,)),
            pltpu.SemaphoreType.DMA((2,)),
            pltpu.SemaphoreType.DMA((levels, 2)),
            pltpu.SemaphoreType.DMA((2,)),
            pltpu.SemaphoreType.DMA((2, n)),
        ],
        compiler_params=pltpu.CompilerParams(
            collective_id=0, has_side_effects=True, vmem_limit_bytes=58000000
        ),
        name="levels",
    )(
        signal.reshape(points // LANES, LANES, columns), col_factor, row_factor, factors, col_leaf_sizes, row_leaf_sizes,
        level_order.reshape(levels, blocks),
    )
    return pl.pallas_call(
        rows_kernel,
        out_shape=jax.ShapeDtypeStruct((points, columns), bf16),
        in_specs=[smem, vmem],
        out_specs=hbm,
        scratch_shapes=[
            pltpu.VMEM((points + reach, columns), bf16),
            pltpu.SemaphoreType.DMA((points // (8 * LANES),)),
        ],
        compiler_params=pltpu.CompilerParams(vmem_limit_bytes=16 << 20),
        name="rows",
    )(row_leaf_sizes, leafwise)


def solution(mesh):
    in_specs = (
        P("blk", "rhs"),
        P(None, "blk"),
        P(None, "blk"),
        P(None, "blk", None, "rhs", None, None),
        P("blk", None),
        P("blk", None),
        P(None, "blk", None),
    )
    return jax.shard_map(
        functools.partial(local, mesh.shape["blk"]),
        mesh=mesh, in_specs=in_specs, out_specs=P("blk", "rhs"), check_vma=False,
    )
```
